256 devices in a mesh: copy: 2 (over core), fsdp: 32 (over z, y), tp: 4 (over x).
Axes of the slice: x: 4, y: 4, z: 8, core: 2. Of those that a mesh axis runs over, the one named last changes fastest.
Arguments:
- gradients: float32 [256, 128, 4096], P('copy', 'fsdp', 'tp'), parts along dimension 0, may hold values from -6 to 6
- momentum: float32 [256, 128, 4096], P('copy', 'fsdp', 'tp'), parts along dimension 0, may hold values from -6 to 6
- weights: float32 [256, 128, 4096], P('copy', 'fsdp', 'tp'), parts along dimension 0, may hold values from -0.1875 to 0.1875
Outputs:
- new_weights: float32 [256, 128, 4096], P('copy', 'fsdp', 'tp'), parts along dimension 0
- new_momentum: float32 [256, 128, 4096], P('copy', 'fsdp', 'tp'), parts along dimension 0
The draws below stay inside these ranges and needn't reach their ends.
There are 2 independent parts, one for each index of `copy`. The reference program is written for one: setup_inputs(seed, part) draws one part's arguments, and reference() takes and returns one part's arrays. A program takes and returns all parts, laid end to end along the dimension named above; each array names one. Nothing has to cross between parts.
All inputs are finite; a program needn't handle non-finite values.
Results may differ from the reference program's by a relative error of at most 0.00014.
Values sent between devices are 32-bit elements; how exact they have to be, the bound alone decides.
A program may use at most 64 MiB of HBM per device.

```python
import jax
import jax.numpy as jnp
from jax import lax

SIDE = 128
WIDE = 4096
MATS = 128
ITERS = 4


def steps_of(stream_key, dims, cuts, low, largest):
    gain, own = 1.0, jax.random.fold_in(stream_key, 6)
    for position, shards_of in cuts:
        steps = jnp.exp(jax.random.uniform(jax.random.fold_in(own, position), (shards_of,), jnp.float32, low / len(cuts), largest / len(cuts)))
        gain = gain * jnp.repeat(steps, dims[position] // shards_of).reshape([-1 if axis == position else 1 for axis in range(len(dims))])
    return gain


def normal_values(key, shape, deviation, reach, shards=(), held_as=jnp.bfloat16):
    factor_of = steps_of(key, shape, shards, -0.22, 0.18) if shards else 1.0
    values = jax.random.normal(key, shape, jnp.float32) * deviation * factor_of
    return jnp.minimum(jnp.maximum(values, -reach), reach).astype(held_as)


def setup_inputs(seed: int = 0, part: int = 0) -> dict:
    arg_keys = jax.random.split(jax.random.key(seed), 4)
    own_keys = jax.random.split(jax.random.fold_in(arg_keys[3], part), 4)
    gradients = normal_values(own_keys[0], (MATS, SIDE, WIDE), 1.0, 6.0, ((1, 32), (2, 4)), jnp.float32)
    momentum = normal_values(own_keys[1], (MATS, SIDE, WIDE), 1.0, 6.0, ((1, 32), (2, 4)), jnp.float32)
    weights = normal_values(own_keys[2], (MATS, SIDE, WIDE), 0.03, 0.1875, ((1, 32), (2, 4)), jnp.float32)
    return dict(gradients=gradients, momentum=momentum, weights=weights)


hold_rate = 0.95
learn_rate = 0.9
decay_rate = 0.1

def reference(gradients, momentum, weights):
    new_momentum = hold_rate * momentum + gradients
    direction = hold_rate * new_momentum + gradients

    def orthogonal_one(stack):
        iterate = stack[None]
        iterate = iterate * lax.rsqrt(lax.optimization_barrier(jnp.sum(iterate * iterate, axis=(1, 2), keepdims=True)) + 1e-06)
        for step in range(ITERS):
            gram = jnp.einsum('mik,mjk->mij', iterate, iterate, precision=lax.Precision.HIGHEST)
            mixed = -4.775 * gram + 2.0315 * jnp.einsum('mij,mjk->mik', gram, gram, precision=lax.Precision.HIGHEST)
            iterate = 3.4445 * iterate + jnp.einsum('mij,mjk->mik', mixed, iterate, precision=lax.Precision.HIGHEST)
        return iterate[0]
    iterate = lax.map(orthogonal_one, direction)
    new_weights = (1.0 - learn_rate * decay_rate) * weights - learn_rate * iterate
    return (new_weights, new_momentum)
```

```python
import functools

import jax
import jax.numpy as jnp
from jax import lax
from jax.experimental import pallas as pl
from jax.experimental.pallas import tpu as pltpu
from jax.sharding import PartitionSpec as P

ITERS = 4

hold_rate = 0.95
learn_rate = 0.9
decay_rate = 0.1

MESH = pl.DeviceIdType.MESH

Z, Y = 8, 4


def ring(step, size):
    return min(step, size - step)


OFFSETS = sorted(
    ((dz, dy) for dz in range(Z) for dy in range(Y) if dz or dy),
    key=lambda o: (-(ring(o[0], Z) + ring(o[1], Y)), o),
)


def dot(a, b, contract=((1,), (0,))):
    return lax.dot_general(
        a,
        b,
        (contract, ((), ())),
        precision=lax.Precision.HIGHEST,
        preferred_element_type=jnp.float32,
    )


def mixing(gram):
    side = gram.shape[0]
    eye = (
        lax.broadcasted_iota(jnp.int32, (side, side), 0)
        == lax.broadcasted_iota(jnp.int32, (side, side), 1)
    ).astype(jnp.float32)
    scale = lax.rsqrt(jnp.sum(gram * eye, keepdims=True) + 1e-06)
    gram = gram * scale * scale
    total = scale * eye
    for step in range(ITERS):
        poly = 3.4445 * eye - 4.775 * gram + 2.0315 * dot(gram, gram)
        total = poly * scale if step == 0 else dot(poly, total)
        if step < ITERS - 1:
            gram = dot(poly, dot(gram, poly))
    return total


def kernel(
    n,
    t,
    grad_hbm,
    mom_hbm,
    weight_hbm,
    new_weight,
    new_mom,
    grad,
    mom,
    weight,
    direction,
    whole,
    grams,
    mixed,
    back,
    load_sem,
    there_send,
    there_recv,
    gram_send,
    gram_recv,
    back_send,
    back_recv,
):
    me, mine = lax.axis_index("fsdp"), lax.axis_index("tp")
    z, y = me // Y, lax.rem(me, Y)
    mats, rows, cols = grad.shape[1:]
    side = n * rows
    steps = range(len(OFFSETS))

    def peer(step, sign=1):
        dz, dy = OFFSETS[step]
        if sign < 0:
            dz, dy = (Z - dz) % Z, (Y - dy) % Y
        return lax.rem(z + dz, Z) * Y + lax.rem(y + dy, Y)

    def tp_peer(step):
        return lax.rem(mine + step, t)

    def load(k, which):
        pairs = ((grad_hbm, grad), (mom_hbm, mom), (weight_hbm, weight))
        source, target = pairs[which]
        return pltpu.make_async_copy(source.at[:, k], target.at[:, k], load_sem.at[which, k])

    def there(k, step):
        return pltpu.make_async_remote_copy(
            src_ref=direction.at[peer(step), k],
            dst_ref=whole.at[k, me],
            send_sem=there_send.at[k, step],
            recv_sem=there_recv.at[k, step],
            device_id={"fsdp": peer(step)},
            device_id_type=MESH,
        )

    def there_landed(k, step):
        return pltpu.make_async_remote_copy(
            src_ref=direction.at[peer(step), k],
            dst_ref=whole.at[k, peer(step, -1)],
            send_sem=there_send.at[k, step],
            recv_sem=there_recv.at[k, step],
            device_id={"fsdp": peer(step)},
            device_id_type=MESH,
        )

    def share(k, step):
        return pltpu.make_async_remote_copy(
            src_ref=grams.at[k, mine],
            dst_ref=grams.at[k, mine],
            send_sem=gram_send.at[k, step],
            recv_sem=gram_recv.at[k, step],
            device_id={"tp": tp_peer(step)},
            device_id_type=MESH,
        )

    def share_landed(k, step):
        return pltpu.make_async_remote_copy(
            src_ref=grams.at[k, mine],
            dst_ref=grams.at[k, tp_peer(t - step)],
            send_sem=gram_send.at[k, step],
            recv_sem=gram_recv.at[k, step],
            device_id={"tp": tp_peer(step)},
            device_id_type=MESH,
        )

    def home(k, step):
        return pltpu.make_async_remote_copy(
            src_ref=mixed.at[k, peer(step)],
            dst_ref=back.at[me, k],
            send_sem=back_send.at[k, step],
            recv_sem=back_recv.at[k, step],
            device_id={"fsdp": peer(step)},
            device_id_type=MESH,
        )

    def home_landed(k, step):
        return pltpu.make_async_remote_copy(
            src_ref=mixed.at[k, peer(step)],
            dst_ref=back.at[peer(step, -1), k],
            send_sem=back_send.at[k, step],
            recv_sem=back_recv.at[k, step],
            device_id={"fsdp": peer(step)},
            device_id_type=MESH,
        )

    barrier = pltpu.get_barrier_semaphore()
    for step in steps:
        pl.semaphore_signal(barrier, inc=1, device_id={"fsdp": peer(step)}, device_id_type=MESH)
    for step in range(1, t):
        pl.semaphore_signal(barrier, inc=1, device_id={"tp": tp_peer(step)}, device_id_type=MESH)
    for k in range(mats):
        load(k, 0).start()
        load(k, 1).start()
    for k in range(mats):
        load(k, 2).start()

    def begin(k):
        load(k, 0).wait()
        load(k, 1).wait()
        fresh = hold_rate * mom[:, k] + grad[:, k]
        new_mom[:, k] = fresh
        direction[:, k] = hold_rate * fresh + grad[:, k]

    for k in range(mats):
        begin(k)
    pl.semaphore_wait(barrier, n + t - 2)

    def send(k, carry):
        for step in steps:
            there(k, step).start()
        whole[k, me] = direction[me, k]
        return carry

    lax.fori_loop(0, mats, send, 0)

    def work(k, carry):
        for step in steps:
            there_landed(k, step).wait_recv()
        matrix = whole[k].reshape(side, cols)
        grams[k, mine] = dot(matrix, matrix, ((1,), (1,)))
        for step in range(1, t):
            share(k, step).start()
        for step in range(1, t):
            share_landed(k, step).wait_recv()
        gram = grams[k, 0]
        for other in range(1, t):
            gram = gram + grams[k, other]
        result = dot(mixing(gram), whole[k].reshape(side, cols))
        mixed[k] = result.reshape(n, rows, cols)
        for step in steps:
            home(k, step).start()
        back[me, k] = mixed[k, me]
        return carry

    lax.fori_loop(0, mats, work, 0)

    def update(k, owner):
        new_weight[owner, k] = (1.0 - learn_rate * decay_rate) * weight[
            owner, k
        ] - learn_rate * back[owner, k]

    def finish(k, carry):
        load(k, 2).wait()
        update(k, me)
        for step in steps:
            home_landed(k, step).wait_recv()
            update(k, peer(step, -1))
        return carry

    lax.fori_loop(0, mats, finish, 0)

    def drain(k, carry):
        for step in steps:
            there(k, step).wait_send()
            home(k, step).wait_send()
        for step in range(1, t):
            share(k, step).wait_send()
        return carry

    lax.fori_loop(0, mats, drain, 0)


def write_kernel(new_weight, new_mom, new_weight_hbm, new_mom_hbm, sem):
    parts = 4
    copies = []
    for which, (source, target) in enumerate(
        ((new_mom, new_mom_hbm), (new_weight, new_weight_hbm))
    ):
        size = source.shape[0] // parts
        for i in range(parts):
            part = pl.ds(i * size, size)
            copies.append(
                pltpu.make_async_copy(source.at[part], target.at[part], sem.at[which, i])
            )
    for copy in copies:
        copy.start()
    for copy in copies:
        copy.wait()


def shards(n, t, gradients, momentum, weights):
    total, rows, cols = gradients.shape
    mats, side = total // n, rows * n
    cut = (n, mats, rows, cols)
    held = pltpu.VMEM(cut, jnp.float32)
    full = pltpu.VMEM((mats, n, rows, cols), jnp.float32)
    sems = lambda *shape: pltpu.SemaphoreType.DMA(shape)
    others = len(OFFSETS)
    new_weights, new_momentum = pl.pallas_call(
        functools.partial(kernel, n, t),
        out_shape=[jax.ShapeDtypeStruct(cut, jnp.float32)] * 2,
        in_specs=[pl.BlockSpec(memory_space=pl.ANY)] * 3,
        out_specs=[pl.BlockSpec(memory_space=pltpu.VMEM)] * 2,
        scratch_shapes=[
            held,
            held,
            held,
            held,
            full,
            pltpu.VMEM((mats, t, side, side), jnp.float32),
            full,
            held,
            sems(3, mats),
            sems(mats, others),
            sems(mats, others),
            sems(mats, t),
            sems(mats, t),
            sems(mats, others),
            sems(mats, others),
        ],
        compiler_params=pltpu.CompilerParams(
            collective_id=0, has_side_effects=True, vmem_limit_bytes=48 * 1024 * 1024
        ),
    )(gradients.reshape(cut), momentum.reshape(cut), weights.reshape(cut))
    new_weights, new_momentum = pl.pallas_call(
        write_kernel,
        out_shape=[jax.ShapeDtypeStruct(cut, jnp.float32)] * 2,
        in_specs=[pl.BlockSpec(memory_space=pl.ANY)] * 2,
        out_specs=[pl.BlockSpec(memory_space=pltpu.HBM)] * 2,
        scratch_shapes=[sems(2, 4)],
        compiler_params=pltpu.CompilerParams(vmem_limit_bytes=1024 * 1024),
    )(new_weights, new_momentum)
    return (new_weights.reshape(total, rows, cols), new_momentum.reshape(total, rows, cols))


def solution(mesh):
    return jax.shard_map(
        functools.partial(shards, mesh.shape["fsdp"], mesh.shape["tp"]),
        mesh=mesh,
        in_specs=(P("copy", "fsdp", "tp"), P("copy", "fsdp", "tp"), P("copy", "fsdp", "tp")),
        out_specs=(P("copy", "fsdp", "tp"), P("copy", "fsdp", "tp")),
        check_vma=False,
    )
```

```python
import functools

import jax
import jax.numpy as jnp
from jax import lax
from jax.experimental import pallas as pl
from jax.experimental.pallas import tpu as pltpu
from jax.sharding import PartitionSpec as P

ITERS = 4

hold_rate = 0.95
learn_rate = 0.9
decay_rate = 0.1

MESH = pl.DeviceIdType.MESH

Z, Y = 8, 4


def ring(step, size):
    return min(step, size - step)


OFFSETS = sorted(
    ((dz, dy) for dz in range(Z) for dy in range(Y) if dz or dy),
    key=lambda o: (-(ring(o[0], Z) + ring(o[1], Y)), o),
)


def dot(a, b, contract=((1,), (0,))):
    return lax.dot_general(
        a,
        b,
        (contract, ((), ())),
        precision=lax.Precision.HIGHEST,
        preferred_element_type=jnp.float32,
    )


def mixing(gram):
    side = gram.shape[0]
    eye = (
        lax.broadcasted_iota(jnp.int32, (side, side), 0)
        == lax.broadcasted_iota(jnp.int32, (side, side), 1)
    ).astype(jnp.float32)
    scale = lax.rsqrt(jnp.sum(gram * eye, keepdims=True) + 1e-06)
    gram = gram * scale * scale
    total = scale * eye
    for step in range(ITERS):
        poly = 3.4445 * eye - 4.775 * gram + 2.0315 * dot(gram, gram)
        total = poly * scale if step == 0 else dot(poly, total)
        if step < ITERS - 1:
            gram = dot(poly, dot(gram, poly))
    return total


def kernel(
    n,
    t,
    grad_hbm,
    mom_hbm,
    weight_hbm,
    new_weight,
    new_mom,
    grad,
    mom,
    weight,
    direction,
    whole,
    grams,
    mixed,
    back,
    load_sem,
    there_send,
    there_recv,
    gram_send,
    gram_recv,
    back_send,
    back_recv,
):
    me, mine = lax.axis_index("fsdp"), lax.axis_index("tp")
    z, y = me // Y, lax.rem(me, Y)
    mats, rows, cols = grad.shape[1:]
    side = n * rows
    steps = range(len(OFFSETS))

    def peer(step):
        dz, dy = OFFSETS[step]
        return lax.rem(z + dz, Z) * Y + lax.rem(y + dy, Y)

    def tp_peer(step):
        return lax.rem(mine + step, t)

    def load(k, which):
        pairs = ((grad_hbm, grad), (mom_hbm, mom), (weight_hbm, weight))
        source, target = pairs[which]
        return pltpu.make_async_copy(source.at[:, k], target.at[:, k], load_sem.at[which, k])

    def there(k, step):
        return pltpu.make_async_remote_copy(
            src_ref=direction.at[peer(step), k],
            dst_ref=whole.at[k, me],
            send_sem=there_send.at[k],
            recv_sem=there_recv.at[k],
            device_id={"fsdp": peer(step)},
            device_id_type=MESH,
        )

    def there_all(k):
        some = pl.ds(0, n - 1)
        return pltpu.make_async_remote_copy(
            src_ref=direction.at[some, k],
            dst_ref=whole.at[k, some],
            send_sem=there_send.at[k],
            recv_sem=there_recv.at[k],
            device_id={"fsdp": peer(0)},
            device_id_type=MESH,
        )

    def share(k, step):
        return pltpu.make_async_remote_copy(
            src_ref=grams.at[k, mine],
            dst_ref=grams.at[k, mine],
            send_sem=gram_send.at[k],
            recv_sem=gram_recv.at[k],
            device_id={"tp": tp_peer(step)},
            device_id_type=MESH,
        )

    def share_all(k):
        some = pl.ds(0, t - 1)
        return pltpu.make_async_remote_copy(
            src_ref=grams.at[k, some],
            dst_ref=grams.at[k, some],
            send_sem=gram_send.at[k],
            recv_sem=gram_recv.at[k],
            device_id={"tp": tp_peer(1)},
            device_id_type=MESH,
        )

    def home(k, step):
        return pltpu.make_async_remote_copy(
            src_ref=mixed.at[k, peer(step)],
            dst_ref=back.at[me, k],
            send_sem=back_send.at[k],
            recv_sem=back_recv.at[k],
            device_id={"fsdp": peer(step)},
            device_id_type=MESH,
        )

    def home_all(k):
        some = pl.ds(0, n - 1)
        return pltpu.make_async_remote_copy(
            src_ref=mixed.at[k, some],
            dst_ref=back.at[some, k],
            send_sem=back_send.at[k],
            recv_sem=back_recv.at[k],
            device_id={"fsdp": peer(0)},
            device_id_type=MESH,
        )

    barrier = pltpu.get_barrier_semaphore()
    for step in steps:
        pl.semaphore_signal(barrier, inc=1, device_id={"fsdp": peer(step)}, device_id_type=MESH)
    for step in range(1, t):
        pl.semaphore_signal(barrier, inc=1, device_id={"tp": tp_peer(step)}, device_id_type=MESH)
    for k in range(mats):
        load(k, 0).start()
        load(k, 1).start()
    for k in range(mats):
        load(k, 2).start()

    def begin(k):
        load(k, 0).wait()
        load(k, 1).wait()
        fresh = hold_rate * mom[:, k] + grad[:, k]
        new_mom[:, k] = fresh
        direction[:, k] = hold_rate * fresh + grad[:, k]

    for k in range(mats):
        begin(k)
    pl.semaphore_wait(barrier, n + t - 2)

    def send(k, carry):
        for step in steps:
            there(k, step).start()
        whole[k, me] = direction[me, k]
        return carry

    lax.fori_loop(0, mats, send, 0)

    def work(k, carry):
        there_all(k).wait_recv()
        matrix = whole[k].reshape(side, cols)
        grams[k, mine] = dot(matrix, matrix, ((1,), (1,)))
        for step in range(1, t):
            share(k, step).start()
        share_all(k).wait_recv()
        gram = grams[k, 0]
        for other in range(1, t):
            gram = gram + grams[k, other]
        result = dot(mixing(gram), whole[k].reshape(side, cols))
        mixed[k] = result.reshape(n, rows, cols)
        for step in steps:
            home(k, step).start()
        back[me, k] = mixed[k, me]
        return carry

    lax.fori_loop(0, mats, work, 0)

    def finish(k, carry):
        load(k, 2).wait()
        there_all(k).wait_send()
        share_all(k).wait_send()
        home_all(k).wait_recv()
        new_weight[:, k] = (1.0 - learn_rate * decay_rate) * weight[:, k] - learn_rate * back[:, k]
        return carry

    lax.fori_loop(0, mats, finish, 0)

    def drain(k, carry):
        home_all(k).wait_send()
        return carry

    lax.fori_loop(0, mats, drain, 0)


def write_kernel(new_weight, new_mom, new_weight_hbm, new_mom_hbm, sem):
    parts = 4
    copies = []
    for which, (source, target) in enumerate(
        ((new_mom, new_mom_hbm), (new_weight, new_weight_hbm))
    ):
        size = source.shape[0] // parts
        for i in range(parts):
            part = pl.ds(i * size, size)
            copies.append(
                pltpu.make_async_copy(source.at[part], target.at[part], sem.at[which, i])
            )
    for copy in copies:
        copy.start()
    for copy in copies:
        copy.wait()


def shards(n, t, gradients, momentum, weights):
    total, rows, cols = gradients.shape
    mats, side = total // n, rows * n
    cut = (n, mats, rows, cols)
    held = pltpu.VMEM(cut, jnp.float32)
    full = pltpu.VMEM((mats, n, rows, cols), jnp.float32)
    sems = lambda *shape: pltpu.SemaphoreType.DMA(shape)
    new_weights, new_momentum = pl.pallas_call(
        functools.partial(kernel, n, t),
        out_shape=[jax.ShapeDtypeStruct(cut, jnp.float32)] * 2,
        in_specs=[pl.BlockSpec(memory_space=pl.ANY)] * 3,
        out_specs=[pl.BlockSpec(memory_space=pltpu.VMEM)] * 2,
        scratch_shapes=[
            held,
            held,
            held,
            held,
            full,
            pltpu.VMEM((mats, t, side, side), jnp.float32),
            full,
            held,
            sems(3, mats),
            sems(mats),
            sems(mats),
            sems(mats),
            sems(mats),
            sems(mats),
            sems(mats),
        ],
        compiler_params=pltpu.CompilerParams(
            collective_id=0, has_side_effects=True, vmem_limit_bytes=48 * 1024 * 1024
        ),
    )(gradients.reshape(cut), momentum.reshape(cut), weights.reshape(cut))
    new_weights, new_momentum = pl.pallas_call(
        write_kernel,
        out_shape=[jax.ShapeDtypeStruct(cut, jnp.float32)] * 2,
        in_specs=[pl.BlockSpec(memory_space=pl.ANY)] * 2,
        out_specs=[pl.BlockSpec(memory_space=pltpu.HBM)] * 2,
        scratch_shapes=[sems(2, 4)],
        compiler_params=pltpu.CompilerParams(vmem_limit_bytes=1024 * 1024),
    )(new_weights, new_momentum)
    return (new_weights.reshape(total, rows, cols), new_momentum.reshape(total, rows, cols))


def solution(mesh):
    return jax.shard_map(
        functools.partial(shards, mesh.shape["fsdp"], mesh.shape["tp"]),
        mesh=mesh,
        in_specs=(P("copy", "fsdp", "tp"), P("copy", "fsdp", "tp"), P("copy", "fsdp", "tp")),
        out_specs=(P("copy", "fsdp", "tp"), P("copy", "fsdp", "tp")),
        check_vma=False,
    )
```

```python
import functools

import jax
import jax.numpy as jnp
from jax import lax
from jax.experimental import pallas as pl
from jax.experimental.pallas import tpu as pltpu
from jax.sharding import PartitionSpec as P

ITERS = 4

hold_rate = 0.95
learn_rate = 0.9
decay_rate = 0.1

MESH = pl.DeviceIdType.MESH

Z, Y = 8, 4


def ring(step, size):
    return min(step, size - step)


OFFSETS = sorted(
    ((dz, dy) for dz in range(Z) for dy in range(Y) if dz or dy),
    key=lambda o: (-(ring(o[0], Z) + ring(o[1], Y)), o),
)


def dot(a, b, contract=((1,), (0,))):
    return lax.dot_general(
        a,
        b,
        (contract, ((), ())),
        precision=lax.Precision.HIGHEST,
        preferred_element_type=jnp.float32,
    )


def mixing(gram):
    side = gram.shape[0]
    eye = (
        lax.broadcasted_iota(jnp.int32, (side, side), 0)
        == lax.broadcasted_iota(jnp.int32, (side, side), 1)
    ).astype(jnp.float32)
    scale = lax.rsqrt(jnp.sum(gram * eye, keepdims=True) + 1e-06)
    gram = gram * scale * scale
    total = scale * eye
    for step in range(ITERS):
        poly = 3.4445 * eye - 4.775 * gram + 2.0315 * dot(gram, gram)
        total = poly * scale if step == 0 else dot(poly, total)
        if step < ITERS - 1:
            gram = dot(poly, dot(gram, poly))
    return total


def kernel(
    n,
    t,
    grad_hbm,
    mom_hbm,
    weight_hbm,
    new_weight,
    new_mom,
    grad,
    mom,
    weight,
    direction,
    whole,
    grams,
    mixed,
    back,
    load_sem,
    there_send,
    there_recv,
    gram_send,
    gram_recv,
    back_send,
    back_recv,
    below,
    above,
    lines,
):
    me, mine = lax.axis_index("fsdp"), lax.axis_index("tp")
    z, y = me // Y, lax.rem(me, Y)
    mats, rows, cols = grad.shape[1:]
    side = n * rows
    steps = range(len(OFFSETS))

    def member(dz, dy):
        return lax.rem(z + dz % Z, Z) * Y + lax.rem(y + dy % Y, Y)

    def peer(step):
        return member(*OFFSETS[step])

    def tp_peer(step):
        return lax.rem(mine + step, t)

    def load(k, which):
        pairs = ((grad_hbm, grad), (mom_hbm, mom), (weight_hbm, weight))
        source, target = pairs[which]
        return pltpu.make_async_copy(source.at[:, k], target.at[:, k], load_sem.at[which, k])

    def there(k, dz, dy):
        return pltpu.make_async_remote_copy(
            src_ref=direction.at[member(dz, dy), k],
            dst_ref=whole.at[k, me],
            send_sem=there_send.at[k],
            recv_sem=there_recv.at[k],
            device_id={"fsdp": member(dz, dy)},
            device_id_type=MESH,
        )

    def there_all(k):
        some = pl.ds(0, n - 1)
        return pltpu.make_async_remote_copy(
            src_ref=direction.at[some, k],
            dst_ref=whole.at[k, some],
            send_sem=there_send.at[k],
            recv_sem=there_recv.at[k],
            device_id={"fsdp": peer(0)},
            device_id_type=MESH,
        )

    def share(k, step):
        return pltpu.make_async_remote_copy(
            src_ref=grams.at[k, mine],
            dst_ref=grams.at[k, mine],
            send_sem=gram_send.at[k],
            recv_sem=gram_recv.at[k],
            device_id={"tp": tp_peer(step)},
            device_id_type=MESH,
        )

    def share_all(k):
        some = pl.ds(0, t - 1)
        return pltpu.make_async_remote_copy(
            src_ref=grams.at[k, some],
            dst_ref=grams.at[k, some],
            send_sem=gram_send.at[k],
            recv_sem=gram_recv.at[k],
            device_id={"tp": tp_peer(1)},
            device_id_type=MESH,
        )

    def home(k, step):
        return pltpu.make_async_remote_copy(
            src_ref=mixed.at[k, peer(step)],
            dst_ref=back.at[me, k],
            send_sem=back_send.at[k],
            recv_sem=back_recv.at[k],
            device_id={"fsdp": peer(step)},
            device_id_type=MESH,
        )

    def home_all(k):
        some = pl.ds(0, n - 1)
        return pltpu.make_async_remote_copy(
            src_ref=mixed.at[k, some],
            dst_ref=back.at[some, k],
            send_sem=back_send.at[k],
            recv_sem=back_recv.at[k],
            device_id={"fsdp": peer(0)},
            device_id_type=MESH,
        )

    def tell(sem, dz, dy):
        pl.semaphore_signal(sem, inc=1, device_id={"fsdp": member(dz, dy)}, device_id_type=MESH)

    def begin(k):
        load(k, 0).wait()
        load(k, 1).wait()
        fresh = hold_rate * mom[:, k] + grad[:, k]
        new_mom[:, k] = fresh
        direction[:, k] = hold_rate * fresh + grad[:, k]

    def along_z(ks, *distances):
        for distance in distances:
            for k in ks:
                there(k, distance, 0).start()

    barrier = pltpu.get_barrier_semaphore()
    for dz, dy in ((1, 0), (-1, 0), (0, 1), (0, -1), (0, 2)):
        tell(barrier, dz, dy)
    for step in range(1, t):
        pl.semaphore_signal(barrier, inc=1, device_id={"tp": tp_peer(step)}, device_id_type=MESH)
    for k in range(mats):
        load(k, 0).start()
        load(k, 1).start()
    for k in range(mats):
        load(k, 2).start()
    begin(0)
    pl.semaphore_wait(barrier, 2 + (Y - 1) + (t - 1))
    tell(below.at[0], 1, 0)
    tell(above.at[0], -1, 0)
    along_z((0,), 1, -1)
    begin(1)
    along_z((1,), 1, -1)
    pl.semaphore_wait(below.at[0], 1)
    tell(below.at[1], 1, 0)
    pl.semaphore_wait(above.at[0], 1)
    tell(above.at[1], -1, 0)
    along_z((0, 1), -2, 2)
    begin(2)
    along_z((2,), 1, -1, -2, 2)
    pl.semaphore_wait(below.at[1], 1)
    tell(below.at[2], 1, 0)
    pl.semaphore_wait(above.at[1], 1)
    along_z((0, 1, 2), -3, 3)
    begin(3)
    along_z((3,), 1, -1, -2, 2, -3, 3)
    pl.semaphore_wait(below.at[2], 1)
    for dy in range(1, Y):
        tell(lines.at[dy - 1], 0, dy)
    along_z(range(mats), Z // 2)
    for dy in range(1, Y):
        for k in range(mats):
            there(k, 0, dy).start()
    for dy in (1, 3, 2):
        pl.semaphore_wait(lines.at[dy - 1], 1)
        for dz, other in OFFSETS:
            if dz and other == Y - dy:
                there(0, dz, other).start()

    def send(k, carry):
        for dz, dy in OFFSETS:
            if dz and dy:
                there(k, dz, dy).start()
        return carry

    lax.fori_loop(1, mats, send, 0)

    def own(k, carry):
        whole[k, me] = direction[me, k]
        return carry

    lax.fori_loop(0, mats, own, 0)

    def work(k, carry):
        there_all(k).wait_recv()
        matrix = whole[k].reshape(side, cols)
        grams[k, mine] = dot(matrix, matrix, ((1,), (1,)))
        for step in range(1, t):
            share(k, step).start()
        share_all(k).wait_recv()
        gram = grams[k, 0]
        for other in range(1, t):
            gram = gram + grams[k, other]
        result = dot(mixing(gram), whole[k].reshape(side, cols))
        mixed[k] = result.reshape(n, rows, cols)
        for step in steps:
            home(k, step).start()
        back[me, k] = mixed[k, me]
        return carry

    lax.fori_loop(0, mats, work, 0)

    def finish(k, carry):
        load(k, 2).wait()
        there_all(k).wait_send()
        share_all(k).wait_send()
        home_all(k).wait_recv()
        new_weight[:, k] = (1.0 - learn_rate * decay_rate) * weight[:, k] - learn_rate * back[:, k]
        return carry

    lax.fori_loop(0, mats, finish, 0)

    def drain(k, carry):
        home_all(k).wait_send()
        return carry

    lax.fori_loop(0, mats, drain, 0)


def write_kernel(new_weight, new_mom, new_weight_hbm, new_mom_hbm, sem):
    parts = 4
    copies = []
    for which, (source, target) in enumerate(
        ((new_mom, new_mom_hbm), (new_weight, new_weight_hbm))
    ):
        size = source.shape[0] // parts
        for i in range(parts):
            part = pl.ds(i * size, size)
            copies.append(
                pltpu.make_async_copy(source.at[part], target.at[part], sem.at[which, i])
            )
    for copy in copies:
        copy.start()
    for copy in copies:
        copy.wait()


def shards(n, t, gradients, momentum, weights):
    total, rows, cols = gradients.shape
    mats, side = total // n, rows * n
    cut = (n, mats, rows, cols)
    held = pltpu.VMEM(cut, jnp.float32)
    full = pltpu.VMEM((mats, n, rows, cols), jnp.float32)
    sems = lambda *shape: pltpu.SemaphoreType.DMA(shape)
    new_weights, new_momentum = pl.pallas_call(
        functools.partial(kernel, n, t),
        out_shape=[jax.ShapeDtypeStruct(cut, jnp.float32)] * 2,
        in_specs=[pl.BlockSpec(memory_space=pl.ANY)] * 3,
        out_specs=[pl.BlockSpec(memory_space=pltpu.VMEM)] * 2,
        scratch_shapes=[
            held,
            held,
            held,
            held,
            full,
            pltpu.VMEM((mats, t, side, side), jnp.float32),
            full,
            held,
            sems(3, mats),
            sems(mats),
            sems(mats),
            sems(mats),
            sems(mats),
            sems(mats),
            sems(mats),
            pltpu.SemaphoreType.REGULAR((Z // 2 - 1,)),
            pltpu.SemaphoreType.REGULAR((Z // 2 - 2,)),
            pltpu.SemaphoreType.REGULAR((Y - 1,)),
        ],
        compiler_params=pltpu.CompilerParams(
            collective_id=0, has_side_effects=True, vmem_limit_bytes=48 * 1024 * 1024
        ),
    )(gradients.reshape(cut), momentum.reshape(cut), weights.reshape(cut))
    new_weights, new_momentum = pl.pallas_call(
        write_kernel,
        out_shape=[jax.ShapeDtypeStruct(cut, jnp.float32)] * 2,
        in_specs=[pl.BlockSpec(memory_space=pl.ANY)] * 2,
        out_specs=[pl.BlockSpec(memory_space=pltpu.HBM)] * 2,
        scratch_shapes=[sems(2, 4)],
        compiler_params=pltpu.CompilerParams(vmem_limit_bytes=1024 * 1024),
    )(new_weights, new_momentum)
    return (new_weights.reshape(total, rows, cols), new_momentum.reshape(total, rows, cols))


def solution(mesh):
    return jax.shard_map(
        functools.partial(shards, mesh.shape["fsdp"], mesh.shape["tp"]),
        mesh=mesh,
        in_specs=(P("copy", "fsdp", "tp"), P("copy", "fsdp", "tp"), P("copy", "fsdp", "tp")),
        out_specs=(P("copy", "fsdp", "tp"), P("copy", "fsdp", "tp")),
        check_vma=False,
    )
```

```python
import functools

import jax
import jax.numpy as jnp
from jax import lax
from jax.experimental import pallas as pl
from jax.experimental.pallas import tpu as pltpu
from jax.sharding import PartitionSpec as P

ITERS = 4

hold_rate = 0.95
learn_rate = 0.9
decay_rate = 0.1

MESH = pl.DeviceIdType.MESH

Z, Y = 8, 4


def ring(step, size):
    return min(step, size - step)


OFFSETS = sorted(
    ((dz, dy) for dz in range(Z) for dy in range(Y) if dz or dy),
    key=lambda o: (-(ring(o[0], Z) + ring(o[1], Y)), o),
)


def dot(a, b, contract=((1,), (0,))):
    return lax.dot_general(
        a,
        b,
        (contract, ((), ())),
        precision=lax.Precision.HIGHEST,
        preferred_element_type=jnp.float32,
    )


def mixing(gram):
    side = gram.shape[0]
    eye = (
        lax.broadcasted_iota(jnp.int32, (side, side), 0)
        == lax.broadcasted_iota(jnp.int32, (side, side), 1)
    ).astype(jnp.float32)
    scale = lax.rsqrt(jnp.sum(gram * eye, keepdims=True) + 1e-06)
    gram = gram * scale * scale
    total = scale * eye
    for step in range(ITERS):
        poly = 3.4445 * eye - 4.775 * gram + 2.0315 * dot(gram, gram)
        total = poly * scale if step == 0 else dot(poly, total)
        if step < ITERS - 1:
            gram = dot(poly, dot(gram, poly))
    return total


def kernel(
    n,
    t,
    grad_hbm,
    mom_hbm,
    weight_hbm,
    new_weight,
    new_mom,
    grad,
    mom,
    weight,
    direction,
    whole,
    grams,
    mixed,
    back,
    load_sem,
    there_send,
    there_recv,
    gram_send,
    gram_recv,
    back_send,
    back_recv,
    below,
    above,
    lines,
):
    me, mine = lax.axis_index("fsdp"), lax.axis_index("tp")
    z, y = me // Y, lax.rem(me, Y)
    mats, rows, cols = grad.shape[1:]
    side = n * rows
    hops = [ring(dz, Z) + ring(dy, Y) for dz, dy in OFFSETS]
    far = [step for step, count in enumerate(hops) if count > 2]
    close = [step for step, count in enumerate(hops) if count <= 2]

    def member(dz, dy):
        return lax.rem(z + dz % Z, Z) * Y + lax.rem(y + dy % Y, Y)

    def peer(step):
        return member(*OFFSETS[step])

    def tp_peer(step):
        return lax.rem(mine + step, t)

    def load(k, which):
        pairs = ((grad_hbm, grad), (mom_hbm, mom), (weight_hbm, weight))
        source, target = pairs[which]
        return pltpu.make_async_copy(source.at[:, k], target.at[:, k], load_sem.at[which, k])

    def there(k, dz, dy):
        return pltpu.make_async_remote_copy(
            src_ref=direction.at[member(dz, dy), k],
            dst_ref=whole.at[k, me],
            send_sem=there_send.at[k],
            recv_sem=there_recv.at[k],
            device_id={"fsdp": member(dz, dy)},
            device_id_type=MESH,
        )

    def there_all(k):
        some = pl.ds(0, n - 1)
        return pltpu.make_async_remote_copy(
            src_ref=direction.at[some, k],
            dst_ref=whole.at[k, some],
            send_sem=there_send.at[k],
            recv_sem=there_recv.at[k],
            device_id={"fsdp": peer(0)},
            device_id_type=MESH,
        )

    def share(k, step):
        return pltpu.make_async_remote_copy(
            src_ref=grams.at[k, mine],
            dst_ref=grams.at[k, mine],
            send_sem=gram_send.at[k],
            recv_sem=gram_recv.at[k],
            device_id={"tp": tp_peer(step)},
            device_id_type=MESH,
        )

    def share_all(k):
        some = pl.ds(0, t - 1)
        return pltpu.make_async_remote_copy(
            src_ref=grams.at[k, some],
            dst_ref=grams.at[k, some],
            send_sem=gram_send.at[k],
            recv_sem=gram_recv.at[k],
            device_id={"tp": tp_peer(1)},
            device_id_type=MESH,
        )

    def home(k, step):
        return pltpu.make_async_remote_copy(
            src_ref=mixed.at[k, peer(step)],
            dst_ref=back.at[me, k],
            send_sem=back_send.at[k],
            recv_sem=back_recv.at[k],
            device_id={"fsdp": peer(step)},
            device_id_type=MESH,
        )

    def home_all(k):
        some = pl.ds(0, n - 1)
        return pltpu.make_async_remote_copy(
            src_ref=mixed.at[k, some],
            dst_ref=back.at[some, k],
            send_sem=back_send.at[k],
            recv_sem=back_recv.at[k],
            device_id={"fsdp": peer(0)},
            device_id_type=MESH,
        )

    def tell(sem, dz, dy):
        pl.semaphore_signal(sem, inc=1, device_id={"fsdp": member(dz, dy)}, device_id_type=MESH)

    def begin(k):
        load(k, 0).wait()
        load(k, 1).wait()
        fresh = hold_rate * mom[:, k] + grad[:, k]
        new_mom[:, k] = fresh
        direction[:, k] = hold_rate * fresh + grad[:, k]

    def along_z(ks, *distances):
        for distance in distances:
            for k in ks:
                there(k, distance, 0).start()

    barrier = pltpu.get_barrier_semaphore()
    for dz, dy in ((1, 0), (-1, 0), (0, 1), (0, -1), (0, 2)):
        tell(barrier, dz, dy)
    for step in range(1, t):
        pl.semaphore_signal(barrier, inc=1, device_id={"tp": tp_peer(step)}, device_id_type=MESH)
    for k in range(mats):
        load(k, 0).start()
        load(k, 1).start()
    for k in range(mats):
        load(k, 2).start()
    begin(0)
    pl.semaphore_wait(barrier, 2 + (Y - 1) + (t - 1))
    tell(below.at[0], 1, 0)
    tell(above.at[0], -1, 0)
    along_z((0,), 1, -1)
    begin(1)
    along_z((1,), 1, -1)
    pl.semaphore_wait(below.at[0], 1)
    tell(below.at[1], 1, 0)
    pl.semaphore_wait(above.at[0], 1)
    tell(above.at[1], -1, 0)
    along_z((0, 1), -2, 2)
    begin(2)
    along_z((2,), 1, -1, -2, 2)
    pl.semaphore_wait(below.at[1], 1)
    tell(below.at[2], 1, 0)
    pl.semaphore_wait(above.at[1], 1)
    along_z((0, 1, 2), -3, 3)
    begin(3)
    along_z((3,), 1, -1, -2, 2, -3, 3)
    pl.semaphore_wait(below.at[2], 1)
    for dy in range(1, Y):
        tell(lines.at[dy - 1], 0, dy)
    along_z(range(mats), Z // 2)
    for dy in range(1, Y):
        for k in range(mats):
            there(k, 0, dy).start()
    for dy in (1, 3, 2):
        pl.semaphore_wait(lines.at[dy - 1], 1)
        for dz, other in OFFSETS:
            if dz and other == Y - dy:
                there(0, dz, other).start()

    def send(k, carry):
        for dz, dy in OFFSETS:
            if dz and dy:
                there(k, dz, dy).start()
        return carry

    lax.fori_loop(1, mats, send, 0)

    def own(k, carry):
        whole[k, me] = direction[me, k]
        return carry

    lax.fori_loop(0, mats, own, 0)

    def work(k, carry):
        there_all(k).wait_recv()
        matrix = whole[k].reshape(side, cols)
        grams[k, mine] = dot(matrix, matrix, ((1,), (1,)))
        for step in range(1, t):
            share(k, step).start()
        share_all(k).wait_recv()
        gram = grams[k, 0]
        for other in range(1, t):
            gram = gram + grams[k, other]
        result = dot(mixing(gram), whole[k].reshape(side, cols))
        mixed[k] = result.reshape(n, rows, cols)
        for step in far:
            home(k, step).start()

        @pl.when(k < mats - 2)
        def _():
            for step in close:
                home(k, step).start()

        @pl.when(k == mats - 1)
        def _():
            for step in close:
                for each in (mats - 2, mats - 1):
                    home(each, step).start()

        back[me, k] = mixed[k, me]
        return carry

    lax.fori_loop(0, mats, work, 0)

    def finish(k, carry):
        load(k, 2).wait()
        there_all(k).wait_send()
        share_all(k).wait_send()
        home_all(k).wait_recv()
        new_weight[:, k] = (1.0 - learn_rate * decay_rate) * weight[:, k] - learn_rate * back[:, k]
        return carry

    lax.fori_loop(0, mats, finish, 0)

    def drain(k, carry):
        home_all(k).wait_send()
        return carry

    lax.fori_loop(0, mats, drain, 0)


def write_kernel(new_weight, new_mom, new_weight_hbm, new_mom_hbm, sem):
    copies = [
        pltpu.make_async_copy(new_mom, new_mom_hbm, sem.at[0]),
        pltpu.make_async_copy(new_weight, new_weight_hbm, sem.at[1]),
    ]
    for copy in copies:
        copy.start()
    for copy in copies:
        copy.wait()


def shards(n, t, gradients, momentum, weights):
    total, rows, cols = gradients.shape
    mats, side = total // n, rows * n
    cut = (n, mats, rows, cols)
    held = pltpu.VMEM(cut, jnp.float32)
    full = pltpu.VMEM((mats, n, rows, cols), jnp.float32)
    sems = lambda *shape: pltpu.SemaphoreType.DMA(shape)
    new_weights, new_momentum = pl.pallas_call(
        functools.partial(kernel, n, t),
        out_shape=[jax.ShapeDtypeStruct(cut, jnp.float32)] * 2,
        in_specs=[pl.BlockSpec(memory_space=pl.ANY)] * 3,
        out_specs=[pl.BlockSpec(memory_space=pltpu.VMEM)] * 2,
        scratch_shapes=[
            held,
            held,
            held,
            held,
            full,
            pltpu.VMEM((mats, t, side, side), jnp.float32),
            full,
            held,
            sems(3, mats),
            sems(mats),
            sems(mats),
            sems(mats),
            sems(mats),
            sems(mats),
            sems(mats),
            pltpu.SemaphoreType.REGULAR((Z // 2 - 1,)),
            pltpu.SemaphoreType.REGULAR((Z // 2 - 2,)),
            pltpu.SemaphoreType.REGULAR((Y - 1,)),
        ],
        compiler_params=pltpu.CompilerParams(
            collective_id=0, has_side_effects=True, vmem_limit_bytes=48 * 1024 * 1024
        ),
    )(gradients.reshape(cut), momentum.reshape(cut), weights.reshape(cut))
    new_weights, new_momentum = pl.pallas_call(
        write_kernel,
        out_shape=[jax.ShapeDtypeStruct(cut, jnp.float32)] * 2,
        in_specs=[pl.BlockSpec(memory_space=pl.ANY)] * 2,
        out_specs=[pl.BlockSpec(memory_space=pltpu.HBM)] * 2,
        scratch_shapes=[sems(2)],
        compiler_params=pltpu.CompilerParams(vmem_limit_bytes=1024 * 1024),
    )(new_weights, new_momentum)
    return (new_weights.reshape(total, rows, cols), new_momentum.reshape(total, rows, cols))


def solution(mesh):
    return jax.shard_map(
        functools.partial(shards, mesh.shape["fsdp"], mesh.shape["tp"]),
        mesh=mesh,
        in_specs=(P("copy", "fsdp", "tp"), P("copy", "fsdp", "tp"), P("copy", "fsdp", "tp")),
        out_specs=(P("copy", "fsdp", "tp"), P("copy", "fsdp", "tp")),
        check_vma=False,
    )
```

```python
import functools

import jax
import jax.numpy as jnp
from jax import lax
from jax.experimental import pallas as pl
from jax.experimental.pallas import tpu as pltpu
from jax.sharding import PartitionSpec as P

ITERS = 4

hold_rate = 0.95
learn_rate = 0.9
decay_rate = 0.1

MESH = pl.DeviceIdType.MESH

Z, Y = 8, 4


def ring(step, size):
    return min(step, size - step)


OFFSETS = sorted(
    ((dz, dy) for dz in range(Z) for dy in range(Y) if dz or dy),
    key=lambda o: (-(ring(o[0], Z) + ring(o[1], Y)), o),
)


def dot(a, b, contract=((1,), (0,))):
    return lax.dot_general(
        a,
        b,
        (contract, ((), ())),
        precision=lax.Precision.HIGHEST,
        preferred_element_type=jnp.float32,
    )


def mixing(gram):
    side = gram.shape[0]
    eye = (
        lax.broadcasted_iota(jnp.int32, (side, side), 0)
        == lax.broadcasted_iota(jnp.int32, (side, side), 1)
    ).astype(jnp.float32)
    scale = lax.rsqrt(jnp.sum(gram * eye, keepdims=True) + 1e-06)
    gram = gram * scale * scale
    total = scale * eye
    for step in range(ITERS):
        poly = 3.4445 * eye - 4.775 * gram + 2.0315 * dot(gram, gram)
        total = poly * scale if step == 0 else dot(poly, total)
        if step < ITERS - 1:
            gram = dot(poly, dot(gram, poly))
    return total


def kernel(
    n,
    t,
    grad_hbm,
    mom_hbm,
    weight_hbm,
    new_weight,
    new_mom,
    grad,
    mom,
    weight,
    direction,
    whole,
    grams,
    mixed,
    back,
    load_sem,
    there_send,
    there_recv,
    gram_send,
    gram_recv,
    back_send,
    back_recv,
    below,
    above,
    lines,
):
    me, mine = lax.axis_index("fsdp"), lax.axis_index("tp")
    z, y = me // Y, lax.rem(me, Y)
    mats, rows, cols = grad.shape[1:]
    side = n * rows
    hops = [ring(dz, Z) + ring(dy, Y) for dz, dy in OFFSETS]
    far = [step for step, count in enumerate(hops) if count > 2]
    close = [step for step, count in enumerate(hops) if count <= 2]

    def member(dz, dy):
        return lax.rem(z + dz % Z, Z) * Y + lax.rem(y + dy % Y, Y)

    def peer(step):
        return member(*OFFSETS[step])

    def tp_peer(step):
        return lax.rem(mine + step, t)

    def load(k, which):
        pairs = ((grad_hbm, grad), (mom_hbm, mom), (weight_hbm, weight))
        source, target = pairs[which]
        return pltpu.make_async_copy(source.at[:, k], target.at[:, k], load_sem.at[which, k])

    def there(k, dz, dy):
        return pltpu.make_async_remote_copy(
            src_ref=direction.at[member(dz, dy), k],
            dst_ref=whole.at[k, me],
            send_sem=there_send.at[k],
            recv_sem=there_recv.at[k],
            device_id={"fsdp": member(dz, dy)},
            device_id_type=MESH,
        )

    def there_all(k):
        some = pl.ds(0, n - 1)
        return pltpu.make_async_remote_copy(
            src_ref=direction.at[some, k],
            dst_ref=whole.at[k, some],
            send_sem=there_send.at[k],
            recv_sem=there_recv.at[k],
            device_id={"fsdp": peer(0)},
            device_id_type=MESH,
        )

    def share(k, step):
        return pltpu.make_async_remote_copy(
            src_ref=grams.at[k, mine],
            dst_ref=grams.at[k, mine],
            send_sem=gram_send.at[k],
            recv_sem=gram_recv.at[k],
            device_id={"tp": tp_peer(step)},
            device_id_type=MESH,
        )

    def share_all(k):
        some = pl.ds(0, t - 1)
        return pltpu.make_async_remote_copy(
            src_ref=grams.at[k, some],
            dst_ref=grams.at[k, some],
            send_sem=gram_send.at[k],
            recv_sem=gram_recv.at[k],
            device_id={"tp": tp_peer(1)},
            device_id_type=MESH,
        )

    def home(k, step):
        return pltpu.make_async_remote_copy(
            src_ref=mixed.at[k, peer(step)],
            dst_ref=back.at[me, k],
            send_sem=back_send.at[k],
            recv_sem=back_recv.at[k],
            device_id={"fsdp": peer(step)},
            device_id_type=MESH,
        )

    def home_all(k):
        some = pl.ds(0, n - 1)
        return pltpu.make_async_remote_copy(
            src_ref=mixed.at[k, some],
            dst_ref=back.at[some, k],
            send_sem=back_send.at[k],
            recv_sem=back_recv.at[k],
            device_id={"fsdp": peer(0)},
            device_id_type=MESH,
        )

    def tell(sem, dz, dy):
        pl.semaphore_signal(sem, inc=1, device_id={"fsdp": member(dz, dy)}, device_id_type=MESH)

    def begin(k):
        load(k, 0).wait()
        load(k, 1).wait()
        fresh = hold_rate * mom[:, k] + grad[:, k]
        new_mom[:, k] = fresh
        direction[:, k] = hold_rate * fresh + grad[:, k]

    def along_z(ks, *distances):
        for distance in distances:
            for k in ks:
                there(k, distance, 0).start()

    barrier = pltpu.get_barrier_semaphore()
    for dz, dy in ((1, 0), (-1, 0), (0, 1), (0, -1), (0, 2)):
        tell(barrier, dz, dy)
    for step in range(1, t):
        pl.semaphore_signal(barrier, inc=1, device_id={"tp": tp_peer(step)}, device_id_type=MESH)
    for k in range(mats):
        load(k, 0).start()
        load(k, 1).start()
    for k in range(mats):
        load(k, 2).start()
    begin(0)
    pl.semaphore_wait(barrier, 2 + (Y - 1) + (t - 1))
    tell(below.at[0], 1, 0)
    tell(above.at[0], -1, 0)
    along_z((0,), 1, -1)
    begin(1)
    along_z((1,), 1, -1)
    pl.semaphore_wait(below.at[0], 1)
    tell(below.at[1], 1, 0)
    pl.semaphore_wait(above.at[0], 1)
    tell(above.at[1], -1, 0)
    along_z((0, 1), -2, 2)
    begin(2)
    along_z((2,), 1, -1, -2, 2)
    pl.semaphore_wait(below.at[1], 1)
    tell(below.at[2], 1, 0)
    pl.semaphore_wait(above.at[1], 1)
    along_z((0, 1, 2), -3, 3)
    begin(3)
    along_z((3,), 1, -1, -2, 2, -3, 3)
    pl.semaphore_wait(below.at[2], 1)
    for dy in range(1, Y):
        tell(lines.at[dy - 1], 0, dy)
    along_z(range(mats), Z // 2)
    for dy in range(1, Y):
        for k in range(mats):
            there(k, 0, dy).start()
    for dy in (1, 3, 2):
        pl.semaphore_wait(lines.at[dy - 1], 1)
        for dz, other in OFFSETS:
            if dz and other == Y - dy:
                there(0, dz, other).start()

    def send(k, carry):
        for dz, dy in OFFSETS:
            if dz and dy:
                there(k, dz, dy).start()
        return carry

    lax.fori_loop(1, mats, send, 0)

    def own(k, carry):
        whole[k, me] = direction[me, k]
        return carry

    lax.fori_loop(0, mats, own, 0)

    def work(k, carry):
        there_all(k).wait_recv()
        matrix = whole[k].reshape(side, cols)
        grams[k, mine] = dot(matrix, matrix, ((1,), (1,)))
        for step in range(1, t):
            share(k, step).start()
        share_all(k).wait_recv()
        gram = grams[k, 0]
        for other in range(1, t):
            gram = gram + grams[k, other]
        result = dot(mixing(gram), whole[k].reshape(side, cols))
        mixed[k] = result.reshape(n, rows, cols)
        for step in far:
            home(k, step).start()

        @pl.when(k < mats - 2)
        def _():
            for step in close:
                home(k, step).start()

        @pl.when(k == mats - 1)
        def _():
            def round_of(first):
                for step in close:
                    @pl.when((peer(step) < Y) == first)
                    def _():
                        for each in (mats - 2, mats - 1):
                            home(each, step).start()

            round_of(True)
            round_of(False)

        back[me, k] = mixed[k, me]
        return carry

    lax.fori_loop(0, mats, work, 0)

    def finish(k, carry):
        load(k, 2).wait()
        there_all(k).wait_send()
        share_all(k).wait_send()
        home_all(k).wait_recv()
        new_weight[:, k] = (1.0 - learn_rate * decay_rate) * weight[:, k] - learn_rate * back[:, k]
        return carry

    lax.fori_loop(0, mats, finish, 0)

    def drain(k, carry):
        home_all(k).wait_send()
        return carry

    lax.fori_loop(0, mats, drain, 0)


def write_kernel(new_weight, new_mom, new_weight_hbm, new_mom_hbm, sem):
    copies = [
        pltpu.make_async_copy(new_mom, new_mom_hbm, sem.at[0]),
        pltpu.make_async_copy(new_weight, new_weight_hbm, sem.at[1]),
    ]
    for copy in copies:
        copy.start()
    for copy in copies:
        copy.wait()


def shards(n, t, gradients, momentum, weights):
    total, rows, cols = gradients.shape
    mats, side = total // n, rows * n
    cut = (n, mats, rows, cols)
    held = pltpu.VMEM(cut, jnp.float32)
    full = pltpu.VMEM((mats, n, rows, cols), jnp.float32)
    sems = lambda *shape: pltpu.SemaphoreType.DMA(shape)
    new_weights, new_momentum = pl.pallas_call(
        functools.partial(kernel, n, t),
        out_shape=[jax.ShapeDtypeStruct(cut, jnp.float32)] * 2,
        in_specs=[pl.BlockSpec(memory_space=pl.ANY)] * 3,
        out_specs=[pl.BlockSpec(memory_space=pltpu.VMEM)] * 2,
        scratch_shapes=[
            held,
            held,
            held,
            held,
            full,
            pltpu.VMEM((mats, t, side, side), jnp.float32),
            full,
            held,
            sems(3, mats),
            sems(mats),
            sems(mats),
            sems(mats),
            sems(mats),
            sems(mats),
            sems(mats),
            pltpu.SemaphoreType.REGULAR((Z // 2 - 1,)),
            pltpu.SemaphoreType.REGULAR((Z // 2 - 2,)),
            pltpu.SemaphoreType.REGULAR((Y - 1,)),
        ],
        compiler_params=pltpu.CompilerParams(
            collective_id=0, has_side_effects=True, vmem_limit_bytes=48 * 1024 * 1024
        ),
    )(gradients.reshape(cut), momentum.reshape(cut), weights.reshape(cut))
    new_weights, new_momentum = pl.pallas_call(
        write_kernel,
        out_shape=[jax.ShapeDtypeStruct(cut, jnp.float32)] * 2,
        in_specs=[pl.BlockSpec(memory_space=pl.ANY)] * 2,
        out_specs=[pl.BlockSpec(memory_space=pltpu.HBM)] * 2,
        scratch_shapes=[sems(2)],
        compiler_params=pltpu.CompilerParams(vmem_limit_bytes=1024 * 1024),
    )(new_weights, new_momentum)
    return (new_weights.reshape(total, rows, cols), new_momentum.reshape(total, rows, cols))


def solution(mesh):
    return jax.shard_map(
        functools.partial(shards, mesh.shape["fsdp"], mesh.shape["tp"]),
        mesh=mesh,
        in_specs=(P("copy", "fsdp", "tp"), P("copy", "fsdp", "tp"), P("copy", "fsdp", "tp")),
        out_specs=(P("copy", "fsdp", "tp"), P("copy", "fsdp", "tp")),
        check_vma=False,
    )
```
